8 devices in a mesh: data: 8 (over z, y, x, core).
Axes of the slice: x: 2, y: 2, z: 1, core: 2. Of those that a mesh axis runs over, the one named last changes fastest.
Arguments:
- w_in: float32 [8192, 2048], replicated
- w_up: float32 [2, 2048, 8192], replicated
- w_down: float32 [2, 8192, 2048], replicated
- mom_in: float32 [8192, 2048], replicated
- mom_up: float32 [2, 2048, 8192], replicated
- mom_down: float32 [2, 8192, 2048], replicated
- x_now: bfloat16 [4096, 8192], P('data')
- y_now: bfloat16 [4096, 2048], P('data')
- x_next: bfloat16 [4096, 8192], P('data')
- y_next: bfloat16 [4096, 2048], P('data')
Outputs:
- output 1: float32 [8192, 2048], replicated
- output 2: float32 [2, 2048, 8192], replicated
- output 3: float32 [2, 8192, 2048], replicated
- output 4: float32 [8192, 2048], replicated
- output 5: float32 [2, 2048, 8192], replicated
- output 6: float32 [2, 8192, 2048], replicated
- output 7: float32 [4096], P('data')
- output 8: float32 [4096, 2048], P('data')
All inputs are finite; a program needn't handle non-finite values.
Results may differ from the reference program's by a relative error of at most 0.0113557.
Values are sent between devices in bfloat16 or wider.
A program may use at most 5.25 GiB of HBM per device.

```python
import jax
import jax.numpy as jnp
from jax import lax

D = 2048
FF = 8192
E = 8192
LAYERS = 2
BATCH_ROWS = 4096
STEP_SIZE = 4.0 * D / (FF * (LAYERS + 1))
MOMENTUM = 0.9


def setup_inputs(seed: int = 0) -> dict:
    key_list = jax.random.split(jax.random.key(seed), 10)
    in_scale = E ** -0.5
    up_scale = D ** -0.5
    down_scale = (FF * LAYERS) ** -0.5
    mom_factor = 0.75 / D
    return {
        "w_in": jax.random.normal(key_list[0], (E, D), jnp.float32) * in_scale,
        "w_up": jax.random.normal(key_list[1], (LAYERS, D, FF), jnp.float32) * up_scale,
        "w_down": jax.random.normal(key_list[2], (LAYERS, FF, D), jnp.float32) * down_scale,
        "mom_in": jax.random.normal(key_list[3], (E, D), jnp.float32) * (in_scale * mom_factor),
        "mom_up": jax.random.normal(key_list[4], (LAYERS, D, FF), jnp.float32) * (up_scale * mom_factor),
        "mom_down": jax.random.normal(key_list[5], (LAYERS, FF, D), jnp.float32) * (down_scale * mom_factor),
        "x_now": jax.random.normal(key_list[6], (BATCH_ROWS, E), jnp.float32).astype(jnp.bfloat16),
        "y_now": jax.random.normal(key_list[7], (BATCH_ROWS, D), jnp.float32).astype(jnp.bfloat16),
        "x_next": jax.random.normal(key_list[8], (BATCH_ROWS, E), jnp.float32).astype(jnp.bfloat16),
        "y_next": jax.random.normal(key_list[9], (BATCH_ROWS, D), jnp.float32).astype(jnp.bfloat16),
    }


def gelu_tanh(pre_value):
    return jax.nn.gelu(pre_value, approximate=True)


def stack_forward(w_in, w_up, w_down, x_rows):
    h_first = jnp.dot(x_rows, w_in.astype(jnp.bfloat16), preferred_element_type=jnp.float32)

    def layer_step(h_state, layer_weights):
        up_mat, down_mat = layer_weights
        h_low = h_state.astype(jnp.bfloat16)
        pre_act = jnp.dot(h_low, up_mat.astype(jnp.bfloat16), preferred_element_type=jnp.float32)
        act_low = gelu_tanh(pre_act).astype(jnp.bfloat16)
        h_state = h_state + jnp.dot(act_low, down_mat.astype(jnp.bfloat16), preferred_element_type=jnp.float32)
        return h_state, h_low

    return lax.scan(layer_step, h_first, (w_up, w_down))


def stack_gradients(w_in, w_up, w_down, x_rows, y_rows):
    h_last, layer_inputs = stack_forward(w_in, w_up, w_down, x_rows)
    cot_last = (h_last - y_rows.astype(jnp.float32)) / (BATCH_ROWS * D)

    def layer_back(cot_state, packed):
        up_mat, down_mat, h_low = packed
        up_low = up_mat.astype(jnp.bfloat16)
        down_low = down_mat.astype(jnp.bfloat16)
        pre_act = jnp.dot(h_low, up_low, preferred_element_type=jnp.float32)
        act_val, gelu_back = jax.vjp(gelu_tanh, pre_act)
        act_low = act_val.astype(jnp.bfloat16)
        cot_low = cot_state.astype(jnp.bfloat16)
        grad_down = jnp.dot(act_low.T, cot_low, preferred_element_type=jnp.float32)
        act_cot = jnp.dot(cot_low, down_low.T, preferred_element_type=jnp.float32)
        pre_cot = gelu_back(act_cot)[0].astype(jnp.bfloat16)
        grad_up = jnp.dot(h_low.T, pre_cot, preferred_element_type=jnp.float32)
        cot_state = cot_state + jnp.dot(pre_cot, up_low.T, preferred_element_type=jnp.float32)
        return cot_state, (grad_up, grad_down)

    cot_first, layer_grads = lax.scan(layer_back, cot_last, (w_up, w_down, layer_inputs), reverse=True)
    grad_in = jnp.dot(x_rows.T, cot_first.astype(jnp.bfloat16), preferred_element_type=jnp.float32)
    return grad_in, layer_grads[0], layer_grads[1]


def reference(w_in, w_up, w_down, mom_in, mom_up, mom_down, x_now, y_now, x_next, y_next):
    grad_in, grad_up, grad_down = stack_gradients(w_in, w_up, w_down, x_now, y_now)
    new_mom_in = MOMENTUM * mom_in + grad_in
    new_mom_up = MOMENTUM * mom_up + grad_up
    new_mom_down = MOMENTUM * mom_down + grad_down
    new_w_in = w_in - STEP_SIZE * new_mom_in
    new_w_up = w_up - STEP_SIZE * new_mom_up
    new_w_down = w_down - STEP_SIZE * new_mom_down
    h_next = stack_forward(new_w_in, new_w_up, new_w_down, x_next)[0]
    loss_next = jnp.sum(jnp.square(h_next - y_next.astype(jnp.float32)), axis=1) / (2 * D)
    return (new_w_in, new_w_up, new_w_down, new_mom_in, new_mom_up, new_mom_down, loss_next, h_next)
```

```python
import functools

import jax
import jax.numpy as jnp
from jax import lax
from jax.experimental import pallas as pl
from jax.experimental.pallas import tpu as pltpu
from jax.sharding import PartitionSpec as P


MOMENTUM = 0.9
BLOCK = 256
STEP_BLOCK = 1024
CHUNK = 256
ROW_CONTRACT = (((0,), (0,)), ((), ()))
COL_CONTRACT = (((1,), (1,)), ((), ()))


def gelu_tanh(pre_value):
    return jax.nn.gelu(pre_value, approximate=True)


class Plan:
    def __init__(self, first, second, size):
        self.first, self.second, self.size = first, second, size
        me = lax.axis_index("data")
        bit = lambda mask: (me // mask) % 2
        self.f, self.s, self.c = bit(first), bit(second), bit(1)

    def quarter(self, flip_f, flip_c):
        f = 1 - self.f if flip_f else self.f
        c = 1 - self.c if flip_c else self.c
        return 2 * f + c

    def piece(self, flip_f, flip_s, flip_c):
        s = 1 - self.s if flip_s else self.s
        return 2 * self.quarter(flip_f, flip_c) + s

    def quarters(self):
        return [self.quarter(1, 0), self.quarter(1, 1), self.quarter(0, 1), self.quarter(0, 0)]

    def hop(self, value, mask):
        return lax.ppermute(value, "data", [(i, i ^ mask) for i in range(self.size)])

    def exchange_wide(self, parts):
        near, across, partner, own = parts
        near = self.hop(near, self.first)
        across = self.hop(across, self.first | 1)
        return [own, self.hop(partner, 1), near, across]

    def exchange_narrow(self, narrow):
        near = self.hop(narrow, self.first)
        return [narrow, self.hop(narrow, 1), near, self.hop(near, 1)]

    def reduce_piece(self, quarter_sum, axis):
        width = quarter_sum.shape[axis] // 2
        send = lax.dynamic_slice_in_dim(quarter_sum, (1 - self.s) * width, width, axis)
        keep = lax.dynamic_slice_in_dim(quarter_sum, self.s * width, width, axis)
        other = self.hop(send, self.second)
        return (keep.astype(jnp.float32) + other.astype(jnp.float32)).astype(jnp.bfloat16)

    def gather(self, own):
        s1 = self.hop(own, self.second)
        f0 = self.hop(own, self.first)
        f1 = self.hop(s1, self.first)
        near = [own, s1, f0, f1]
        far = [self.hop(value, 1) for value in near]
        flips = [(0, 0), (0, 1), (1, 0), (1, 1)]
        tagged = [(near[i], self.piece(*flips[i], 0)) for i in range(4)]
        tagged += [(far[i], self.piece(*flips[i], 1)) for i in range(4)]
        return [[tagged[i] for i in pair] for pair in ((0, 4), (1, 2), (5, 6), (3, 7))]


def run(kernel, table, operands, in_specs, out_shape, out_specs, steps, work, scratch=(), aliases=None):
    return pl.pallas_call(
        kernel,
        grid_spec=pltpu.PrefetchScalarGridSpec(
            num_scalar_prefetch=1, grid=(steps,), in_specs=in_specs, out_specs=out_specs, scratch_shapes=list(scratch)
        ),
        out_shape=out_shape,
        input_output_aliases=aliases or {},
        compiler_params=pltpu.CompilerParams(dimension_semantics=("arbitrary",)),
        cost_estimate=pl.CostEstimate(flops=work[0], bytes_accessed=work[1], transcendentals=0),
    )(table, *operands)


def lower(ref):
    return ref[...].reshape(ref.shape[-2:]).astype(jnp.bfloat16)


def store_part(step, per, part_refs, value):
    for idx, ref in enumerate(part_refs):

        @pl.when((step >= idx * per) & (step < (idx + 1) * per))
        def _(ref=ref):
            ref[...] = value


def part_specs(count, per, shape, axis):
    def at(idx):
        def block(i, t):
            place = jnp.clip(i - idx * per, 0, per - 1)
            return (place, 0) if axis == 0 else (0, place)

        return block

    return [pl.BlockSpec(shape, at(idx)) for idx in range(count)]


def split_kernel(table_ref, x_ref, *out_refs):
    store_part(pl.program_id(0), 1, out_refs, x_ref[...])


def split_cols(x, table, width):
    rows, count = x.shape[0], table.shape[0]
    shape = (rows, width)
    return run(
        split_kernel, table, [x],
        [pl.BlockSpec(shape, lambda i, t: (0, t[i]))],
        [jax.ShapeDtypeStruct(shape, x.dtype)] * count,
        part_specs(count, 1, shape, 1),
        count, (0, 4 * x.size),
    )


def up_kernel(per, table_ref, p_ref, w_ref, u_ref, *act_refs):
    values = []
    for lo in range(0, STEP_BLOCK, CHUNK):
        low = w_ref[0, :, lo : lo + CHUNK].astype(jnp.bfloat16)
        pre = jnp.dot(p_ref[...], low, preferred_element_type=jnp.float32)
        u_ref[:, lo : lo + CHUNK] = pre
        values.append(gelu_tanh(pre).astype(jnp.bfloat16))
    store_part(pl.program_id(0), per, act_refs, jnp.concatenate(values, axis=1))


def up_forward(p, w, layer, quarters):
    (rows, depth), inner = p.shape, w.shape[2]
    per = inner // 4 // STEP_BLOCK
    block = lambda i, t: t[i // per] * per + i % per
    return run(
        functools.partial(up_kernel, per), jnp.stack(quarters), [p, w],
        [
            pl.BlockSpec((rows, depth), lambda i, t: (0, 0)),
            pl.BlockSpec((1, depth, STEP_BLOCK), lambda i, t: (layer, 0, block(i, t))),
        ],
        [jax.ShapeDtypeStruct((rows, inner), jnp.float32)] + [jax.ShapeDtypeStruct((rows, inner // 4), jnp.bfloat16)] * 4,
        [pl.BlockSpec((rows, STEP_BLOCK), lambda i, t: (0, block(i, t)))] + part_specs(4, per, (rows, STEP_BLOCK), 1),
        4 * per, (2 * rows * depth * inner, 4 * depth * inner + 6 * rows * inner),
    )


def dot_nt(lhs, rhs):
    return lax.dot_general(lhs, rhs, COL_CONTRACT, preferred_element_type=jnp.float32)


def back_kernel(per, table_ref, c_ref, w_ref, u_ref, *q_refs):
    values = []
    for lo in range(0, STEP_BLOCK, CHUNK):
        act_cot = dot_nt(c_ref[...], w_ref[0, lo : lo + CHUNK, :].astype(jnp.bfloat16))
        gelu_back = jax.vjp(gelu_tanh, u_ref[:, lo : lo + CHUNK])[1]
        values.append(gelu_back(act_cot)[0].astype(jnp.bfloat16))
    store_part(pl.program_id(0), per, q_refs, jnp.concatenate(values, axis=1))


def down_backward(c, w, layer, u, quarters):
    (rows, width), inner = c.shape, w.shape[1]
    per = inner // 4 // STEP_BLOCK
    block = lambda i, t: t[i // per] * per + i % per
    return run(
        functools.partial(back_kernel, per), jnp.stack(quarters), [c, w, u],
        [
            pl.BlockSpec((rows, width), lambda i, t: (0, 0)),
            pl.BlockSpec((1, STEP_BLOCK, width), lambda i, t: (layer, block(i, t), 0)),
            pl.BlockSpec((rows, STEP_BLOCK), lambda i, t: (0, block(i, t))),
        ],
        [jax.ShapeDtypeStruct((rows, inner // 4), jnp.bfloat16)] * 4,
        part_specs(4, per, (rows, STEP_BLOCK), 1),
        4 * per, (2 * rows * width * inner, 4 * width * inner + 6 * rows * inner),
    )


def add_kernel(per, transposed, table_ref, base_ref, w_ref, *refs):
    *part_refs, out_ref = refs
    step = pl.program_id(0)

    @pl.when(step == 0)
    def _():
        out_ref[...] = base_ref[...]

    lhs = select_piece(step, per, part_refs)
    if transposed:
        out_ref[...] += dot_nt(lhs, lower(w_ref))
    else:
        out_ref[...] += jnp.dot(lhs, lower(w_ref), preferred_element_type=jnp.float32)


def add_product(base, parts, w, layer, quarters, transposed):
    rows, width = base.shape
    inner = 4 * parts[0].shape[1]
    per = inner // 4 // STEP_BLOCK
    block = lambda i, t: t[i // per] * per + i % per
    whole = pl.BlockSpec((rows, width), lambda i, t: (0, 0))
    if transposed:
        w_spec = pl.BlockSpec((1, width, STEP_BLOCK), lambda i, t: (layer, 0, block(i, t)))
    else:
        w_spec = pl.BlockSpec((1, STEP_BLOCK, width), lambda i, t: (layer, block(i, t), 0))
    return run(
        functools.partial(add_kernel, per, transposed), jnp.stack(quarters), [base, w, *parts],
        [whole, w_spec] + part_specs(4, per, (rows, STEP_BLOCK), 1),
        jax.ShapeDtypeStruct((rows, width), jnp.float32),
        whole,
        4 * per, (2 * rows * width * inner, 4 * width * inner + 2 * rows * inner),
    )


def in_kernel(table_ref, x_ref, w_ref, out_ref):
    term = jnp.dot(x_ref[...], lower(w_ref), preferred_element_type=jnp.float32)

    @pl.when(pl.program_id(0) == 0)
    def _():
        out_ref[...] = term

    @pl.when(pl.program_id(0) != 0)
    def _():
        out_ref[...] += term


def in_forward(x, w, table):
    (rows, depth), width = x.shape, w.shape[1]
    return run(
        in_kernel, table, [x, w],
        [pl.BlockSpec((rows, STEP_BLOCK), lambda i, t: (0, i)), pl.BlockSpec((STEP_BLOCK, width), lambda i, t: (i, 0))],
        jax.ShapeDtypeStruct((rows, width), jnp.float32),
        pl.BlockSpec((rows, width), lambda i, t: (0, 0)),
        depth // STEP_BLOCK, (2 * rows * depth * width, 4 * depth * width + 2 * rows * depth),
    )


def select_piece(step, steps_per_piece, piece_refs):
    value = piece_refs[0][...]
    for idx in range(1, len(piece_refs)):
        value = jnp.where(step >= idx * steps_per_piece, piece_refs[idx][...], value)
    return value


def updated(w_ref, m_ref, grad, step_size):
    new_m = MOMENTUM * m_ref[...] + grad.astype(jnp.float32).reshape(m_ref.shape)
    new_w = w_ref[...] - step_size * new_m
    return new_w, new_m


def rows_kernel(count, per, step_size, has_h, has_old, *refs):
    refs = list(refs)
    refs.pop(0)
    x_ref = refs.pop(0)
    w_ref, m_ref = refs.pop(0), refs.pop(0)
    pieces = [refs.pop(0) for _ in range(count)]
    h_ref = refs.pop(0) if has_h else None
    if has_old:
        refs.pop(0), refs.pop(0)
    new_w_ref, new_m_ref, out_ref = refs
    step = pl.program_id(0)
    new_w, new_m = updated(w_ref, m_ref, select_piece(step, per, pieces), step_size)
    new_w_ref[...] = new_w
    new_m_ref[...] = new_m
    low = new_w.reshape(new_w.shape[-2:]).astype(jnp.bfloat16)
    term = jnp.dot(x_ref[...], low, preferred_element_type=jnp.float32)

    @pl.when(step == 0)
    def _():
        out_ref[...] = term + h_ref[...] if has_h else term

    @pl.when(step != 0)
    def _():
        out_ref[...] += term


def update_rows(x, w, m, layer, pieces, bases, h, old, step_size):
    count, rows = len(pieces), x.shape[0]
    height, width = pieces[0].shape
    per = height // BLOCK
    stacked = w.ndim == 3
    table = jnp.stack(bases) * per

    def where(i, t):
        return t[i // per] + i % per

    lead = (1,) if stacked else ()
    at = (lambda i, t: (layer, where(i, t), 0)) if stacked else (lambda i, t: (where(i, t), 0))
    w_spec = pl.BlockSpec(lead + (BLOCK, width), at)
    in_specs = [pl.BlockSpec((rows, BLOCK), lambda i, t: (0, where(i, t))), w_spec, w_spec]
    in_specs += [
        pl.BlockSpec((BLOCK, width), lambda i, t, j=j: (jnp.clip(i - j * per, 0, per - 1), 0)) for j in range(count)
    ]
    h_spec = pl.BlockSpec((rows, width), lambda i, t: (0, 0))
    operands = [x, w, m, *pieces]
    aliases = {}
    if h is not None:
        operands.append(h)
        in_specs.append(h_spec)
    if old is not None:
        aliases = {len(operands) + 1: 0, len(operands) + 2: 1}
        operands += list(old)
        in_specs += [pl.BlockSpec(memory_space=pl.ANY)] * 2
    steps = count * per
    size = steps * BLOCK * width
    full = jax.ShapeDtypeStruct(w.shape, jnp.float32)
    new_w, new_m, out = run(
        functools.partial(rows_kernel, count, per, step_size, h is not None, old is not None), table, operands,
        in_specs, [full, full, jax.ShapeDtypeStruct((rows, width), jnp.float32)], [w_spec, w_spec, h_spec],
        steps, (2 * rows * size, 18 * size), aliases=aliases,
    )
    return (new_w, new_m), out


def cols_kernel(count, per, step_size, has_old, *refs):
    refs = list(refs)
    refs.pop(0)
    h_ref = refs.pop(0)
    w_ref, m_ref = refs.pop(0), refs.pop(0)
    pieces = [refs.pop(0) for _ in range(count)]
    new_w_ref, new_m_ref, act_ref, low_ref = refs[has_old:]
    step = pl.program_id(0)

    @pl.when(step == 0)
    def _():
        low_ref[...] = h_ref[...].astype(jnp.bfloat16)

    new_w, new_m = updated(w_ref, m_ref, select_piece(step, per, pieces), step_size)
    new_w_ref[...] = new_w
    new_m_ref[...] = new_m
    low = new_w.reshape(new_w.shape[-2:]).astype(jnp.bfloat16)
    pre = jnp.dot(low_ref[...], low, preferred_element_type=jnp.float32)
    act_ref[...] = gelu_tanh(pre).astype(jnp.bfloat16)


def update_cols(h, w, m, layer, pieces, bases, old, step_size):
    count, rows = len(pieces), h.shape[0]
    depth, width = pieces[0].shape
    per = width // BLOCK
    table = jnp.stack(bases) * per

    def where(i, t):
        return t[i // per] + i % per

    w_spec = pl.BlockSpec((1, depth, BLOCK), lambda i, t: (layer, 0, where(i, t)))
    a_spec = pl.BlockSpec((rows, BLOCK), lambda i, t: (0, where(i, t)))
    in_specs = [pl.BlockSpec((rows, depth), lambda i, t: (0, 0)), w_spec, w_spec]
    in_specs += [
        pl.BlockSpec((depth, BLOCK), lambda i, t, j=j: (0, jnp.clip(i - j * per, 0, per - 1))) for j in range(count)
    ]
    operands = [h, w, m, *pieces]
    aliases = {}
    kept = [(out_idx, value) for out_idx, value in enumerate(old) if value is not None]
    for out_idx, value in kept:
        aliases[len(operands) + 1] = out_idx
        operands.append(value)
        in_specs.append(pl.BlockSpec(memory_space=pl.ANY))
    steps = count * per
    size = steps * BLOCK * depth
    full = jax.ShapeDtypeStruct(w.shape, jnp.float32)
    new_w, new_m, act = run(
        functools.partial(cols_kernel, count, per, step_size, len(kept)), table, operands,
        in_specs, [full, full, jax.ShapeDtypeStruct((rows, w.shape[2]), jnp.bfloat16)], [w_spec, w_spec, a_spec],
        steps, (2 * rows * size, 18 * size), [pltpu.VMEM((rows, depth), jnp.bfloat16)], aliases,
    )
    return (new_w, new_m), act


def solution(mesh):
    group_size = mesh.shape["data"]

    def device_steps(w_in, w_up, w_down, mom_in, mom_up, mom_down, x_now, y_now, x_next, y_next):
        local_rows, model_width = y_now.shape
        layer_count = w_up.shape[0]
        inner = w_up.shape[2]
        step_size = 4.0 * model_width / (inner * (layer_count + 1))
        along_x, along_y = Plan(2, 4, group_size), Plan(4, 2, group_size)
        half = x_now.shape[1] // 2

        quarters_x, quarters_y = along_x.quarters(), along_y.quarters()
        halves = quarters_x + [4 + idx for idx in quarters_y]
        x_parts = split_cols(x_now, jnp.stack(halves), half // 4)
        in_wide = [along_x.exchange_wide(x_parts[:4]), along_y.exchange_wide(x_parts[4:])]

        h_state = in_forward(x_now, w_in, jnp.stack(halves))
        saved = []
        for layer in range(layer_count):
            h_low = h_state.astype(jnp.bfloat16)
            up_near = along_y.exchange_narrow(h_low)
            pre_act, *act_parts = up_forward(h_low, w_up, layer, quarters_x)
            down_wide = along_x.exchange_wide(act_parts)
            h_state = add_product(h_state, act_parts, w_down, layer, quarters_x, False)
            saved.append((up_near, down_wide, pre_act))
        cot_state = (h_state - y_now.astype(jnp.float32)) / (local_rows * group_size * model_width)

        def share(lhs, rhs):
            lhs, rhs = jnp.concatenate(lhs), jnp.concatenate(rhs)
            value = lax.dot_general(lhs, rhs, ROW_CONTRACT, preferred_element_type=jnp.float32)
            return value.astype(jnp.bfloat16)

        factors = [None] * layer_count
        for layer in reversed(range(layer_count)):
            up_near, down_wide, pre_act = saved[layer]
            cot_low = cot_state.astype(jnp.bfloat16)
            cot_near = along_x.exchange_narrow(cot_low)
            pre_parts = down_backward(cot_low, w_down, layer, pre_act, quarters_y)
            pre_wide = along_y.exchange_wide(pre_parts)
            cot_state = add_product(cot_state, pre_parts, w_up, layer, quarters_y, True)
            factors[layer] = (down_wide, cot_near, up_near, pre_wide)
        cot_low = cot_state.astype(jnp.bfloat16)
        cot_near = [along_x.exchange_narrow(cot_low), along_y.exchange_narrow(cot_low)]

        up_sums, down_sums, in_sums = [None] * layer_count, [None] * layer_count, [None] * 2
        for layer in reversed(range(layer_count)):
            down_wide, near, up_near, pre_wide = factors[layer]
            up_sums[layer] = along_y.reduce_piece(share(up_near, pre_wide), 1)
            down_sums[layer] = along_x.reduce_piece(share(down_wide, near), 0)
        for part, plan in enumerate((along_x, along_y)):
            in_sums[part] = plan.reduce_piece(share(in_wide[part], cot_near[part]), 0)

        h_state, new_in, new_up, new_down = None, None, None, None
        groups = [plan.gather(own) for plan, own in zip((along_x, along_y), in_sums)]
        for idx in range(4):
            tagged = groups[0][idx] + [(value, base + 8) for value, base in groups[1][idx]]
            pieces, bases = zip(*tagged)
            new_in, h_state = update_rows(x_next, w_in, mom_in, 0, pieces, bases, h_state, new_in, step_size)
        for layer in range(layer_count):
            act_low = None
            for tagged in along_y.gather(up_sums[layer]):
                pieces, bases = zip(*tagged)
                old = (None, None, act_low) if new_up is None else (*new_up, act_low)
                new_up, act_low = update_cols(h_state, w_up, mom_up, layer, pieces, bases, old, step_size)
            for tagged in along_x.gather(down_sums[layer]):
                pieces, bases = zip(*tagged)
                new_down, h_state = update_rows(
                    act_low, w_down, mom_down, layer, pieces, bases, h_state, new_down, step_size
                )
        loss_next = jnp.sum(jnp.square(h_state - y_next.astype(jnp.float32)), axis=1) / (2 * model_width)
        return (new_in[0], new_up[0], new_down[0], new_in[1], new_up[1], new_down[1], loss_next, h_state)

    param_spec = P()
    row_spec = P("data", None)

    return jax.shard_map(
        device_steps,
        mesh=mesh,
        in_specs=(param_spec,) * 6 + (row_spec,) * 4,
        out_specs=(param_spec,) * 6 + (P("data"), row_spec),
        check_vma=False,
    )
```

```python
import functools

import jax
import jax.numpy as jnp
from jax import lax
from jax.experimental import pallas as pl
from jax.experimental.pallas import tpu as pltpu
from jax.sharding import PartitionSpec as P


MOMENTUM = 0.9
BLOCK = 256
CHUNK = 256
UPDATE_ORDER = ((1, 0), (0, 0), (1, 1), (0, 1), (1, 2), (0, 2), (1, 3), (0, 3))
ROW_CONTRACT = (((0,), (0,)), ((), ()))
COL_CONTRACT = (((1,), (1,)), ((), ()))


def gelu_tanh(pre_value):
    return jax.nn.gelu(pre_value, approximate=True)


class Plan:
    def __init__(self, first, second, size):
        self.first, self.second, self.size = first, second, size
        me = lax.axis_index("data")
        self.s = (me // second) % 2
        self.bits = {mask: (me // mask) % 2 for mask in (1, 2, 4)}

    def piece(self, flip_f, flip_s, flip_c):
        flips = {self.first: flip_f, self.second: flip_s, 1: flip_c}
        c, x, y = (1 - self.bits[mask] if flips[mask] else self.bits[mask] for mask in (1, 2, 4))
        return 4 * c + 2 * x + y

    def eighths(self):
        pairs = []
        for flip_f, flip_c in ((1, 0), (1, 1), (0, 1), (0, 0)):
            ours, other = self.piece(flip_f, 0, flip_c), self.piece(flip_f, 1, flip_c)
            pairs += [jnp.where(self.s == 0, ours, other), jnp.where(self.s == 0, other, ours)]
        return pairs

    def hop(self, value, mask):
        return lax.ppermute(value, "data", [(i, i ^ mask) for i in range(self.size)])

    def exchange_wide(self, parts):
        near, across, partner, own = parts
        near = self.hop(near, self.first)
        across = self.hop(across, self.first | 1)
        return [own, self.hop(partner, 1), near, across]

    def exchange_narrow(self, narrow):
        near = self.hop(narrow, self.first)
        return [narrow, self.hop(narrow, 1), near, self.hop(near, 1)]

    def reduce_piece(self, quarter_sum, axis):
        width = quarter_sum.shape[axis] // 2
        send = lax.dynamic_slice_in_dim(quarter_sum, (1 - self.s) * width, width, axis)
        keep = lax.dynamic_slice_in_dim(quarter_sum, self.s * width, width, axis)
        other = self.hop(send, self.second)
        return (keep.astype(jnp.float32) + other.astype(jnp.float32)).astype(jnp.bfloat16)

    def gather(self, own):
        s1 = self.hop(own, self.second)
        f0 = self.hop(own, self.first)
        f1 = self.hop(s1, self.first)
        near = [own, s1, f0, f1]
        far = [self.hop(value, 1) for value in near]
        flips = [(0, 0), (0, 1), (1, 0), (1, 1)]
        tagged = [(near[i], self.piece(*flips[i], 0)) for i in range(4)]
        tagged += [(far[i], self.piece(*flips[i], 1)) for i in range(4)]
        return [[tagged[i] for i in pair] for pair in ((0, 4), (1, 2), (5, 6), (3, 7))]


def run(kernel, table, operands, in_specs, out_shape, out_specs, steps, work, scratch=(), aliases=None):
    return pl.pallas_call(
        kernel,
        grid_spec=pltpu.PrefetchScalarGridSpec(
            num_scalar_prefetch=1, grid=(steps,), in_specs=in_specs, out_specs=out_specs, scratch_shapes=list(scratch)
        ),
        out_shape=out_shape,
        input_output_aliases=aliases or {},
        compiler_params=pltpu.CompilerParams(dimension_semantics=("arbitrary",)),
        cost_estimate=pl.CostEstimate(flops=work[0], bytes_accessed=work[1], transcendentals=0),
    )(table, *operands)


def store_part(step, per, part_refs, value):
    for idx, ref in enumerate(part_refs):

        @pl.when((step >= idx * per) & (step < (idx + 1) * per))
        def _(ref=ref):
            ref[...] = value


def part_specs(count, per, shape, axis):
    def at(idx):
        def block(i, t):
            place = jnp.clip(i - idx * per, 0, per - 1)
            return (place, 0) if axis == 0 else (0, place)

        return block

    return [pl.BlockSpec(shape, at(idx)) for idx in range(count)]


def split_kernel(table_ref, x_ref, *out_refs):
    store_part(pl.program_id(0), 2, out_refs, x_ref[...])


def split_cols(x, table, count):
    rows, size = x.shape[0], x.shape[1] // (2 * count)
    return run(
        split_kernel, table, [x],
        [pl.BlockSpec((rows, size), lambda i, t: (0, t[i]))],
        [jax.ShapeDtypeStruct((rows, 2 * size), x.dtype)] * count,
        part_specs(count, 2, (rows, size), 1),
        2 * count, (0, 4 * x.size),
    )


def up_kernel(per, table_ref, p_ref, w_ref, u_ref, *act_refs):
    values = []
    for lo in range(0, w_ref.shape[2], CHUNK):
        low = w_ref[0, :, lo : lo + CHUNK].astype(jnp.bfloat16)
        pre = jnp.dot(p_ref[...], low, preferred_element_type=jnp.float32)
        u_ref[:, lo : lo + CHUNK] = pre
        values.append(gelu_tanh(pre).astype(jnp.bfloat16))
    store_part(pl.program_id(0), per, act_refs, jnp.concatenate(values, axis=1))


def up_forward(p, w, layer, eighths):
    (rows, depth), inner = p.shape, w.shape[2]
    per, size = 2, inner // 8
    block = lambda i, t: t[i]
    return run(
        functools.partial(up_kernel, per), jnp.stack(eighths), [p, w],
        [
            pl.BlockSpec((rows, depth), lambda i, t: (0, 0)),
            pl.BlockSpec((1, depth, size), lambda i, t: (layer, 0, block(i, t))),
        ],
        [jax.ShapeDtypeStruct((rows, inner), jnp.float32)] + [jax.ShapeDtypeStruct((rows, inner // 4), jnp.bfloat16)] * 4,
        [pl.BlockSpec((rows, size), lambda i, t: (0, block(i, t)))] + part_specs(4, per, (rows, size), 1),
        4 * per, (2 * rows * depth * inner, 4 * depth * inner + 6 * rows * inner),
    )


def dot_nt(lhs, rhs):
    return lax.dot_general(lhs, rhs, COL_CONTRACT, preferred_element_type=jnp.float32)


def back_kernel(per, table_ref, c_ref, w_ref, u_ref, *q_refs):
    values = []
    for lo in range(0, w_ref.shape[1], CHUNK):
        act_cot = dot_nt(c_ref[...], w_ref[0, lo : lo + CHUNK, :].astype(jnp.bfloat16))
        gelu_back = jax.vjp(gelu_tanh, u_ref[:, lo : lo + CHUNK])[1]
        values.append(gelu_back(act_cot)[0].astype(jnp.bfloat16))
    store_part(pl.program_id(0), per, q_refs, jnp.concatenate(values, axis=1))


def down_backward(c, w, layer, u, eighths):
    (rows, width), inner = c.shape, w.shape[1]
    per, size = 2, inner // 8
    block = lambda i, t: t[i]
    return run(
        functools.partial(back_kernel, per), jnp.stack(eighths), [c, w, u],
        [
            pl.BlockSpec((rows, width), lambda i, t: (0, 0)),
            pl.BlockSpec((1, size, width), lambda i, t: (layer, block(i, t), 0)),
            pl.BlockSpec((rows, size), lambda i, t: (0, block(i, t))),
        ],
        [jax.ShapeDtypeStruct((rows, inner // 4), jnp.bfloat16)] * 4,
        part_specs(4, per, (rows, size), 1),
        4 * per, (2 * rows * width * inner, 4 * width * inner + 6 * rows * inner),
    )


def add_kernel(per, transposed, table_ref, base_ref, w_ref, *refs):
    *part_refs, out_ref, low_ref = refs
    step = pl.program_id(0)

    @pl.when(step == 0)
    def _():
        out_ref[...] = base_ref[...]

    lhs = select_piece(step, per, part_refs)
    for lo in range(0, out_ref.shape[1], 2 * CHUNK):
        at = slice(lo, lo + 2 * CHUNK)
        if transposed:
            out_ref[:, at] += dot_nt(lhs, w_ref[0, at, :].astype(jnp.bfloat16))
        else:
            out_ref[:, at] += jnp.dot(lhs, w_ref[0, :, at].astype(jnp.bfloat16), preferred_element_type=jnp.float32)

    @pl.when(step == pl.num_programs(0) - 1)
    def _():
        low_ref[...] = out_ref[...].astype(jnp.bfloat16)


def add_product(base, parts, w, layer, eighths, transposed):
    rows, width = base.shape
    inner = 4 * parts[0].shape[1]
    per, size = 2, inner // 8
    block = lambda i, t: t[i]
    whole = pl.BlockSpec((rows, width), lambda i, t: (0, 0))
    if transposed:
        w_spec = pl.BlockSpec((1, width, size), lambda i, t: (layer, 0, block(i, t)))
    else:
        w_spec = pl.BlockSpec((1, size, width), lambda i, t: (layer, block(i, t), 0))
    return run(
        functools.partial(add_kernel, per, transposed), jnp.stack(eighths), [base, w, *parts],
        [whole, w_spec] + part_specs(4, per, (rows, size), 1),
        [jax.ShapeDtypeStruct((rows, width), dtype) for dtype in (jnp.float32, jnp.bfloat16)],
        [whole, whole],
        4 * per, (2 * rows * width * inner, 4 * width * inner + 2 * rows * inner),
    )


def in_kernel(table_ref, x_ref, w_ref, out_ref, low_ref):
    @pl.when(pl.program_id(0) == 0)
    def _():
        out_ref[...] = jnp.zeros_like(out_ref)

    for lo in range(0, out_ref.shape[1], 2 * CHUNK):
        at = slice(lo, lo + 2 * CHUNK)
        out_ref[:, at] += jnp.dot(x_ref[...], w_ref[:, at].astype(jnp.bfloat16), preferred_element_type=jnp.float32)

    @pl.when(pl.program_id(0) == pl.num_programs(0) - 1)
    def _():
        low_ref[...] = out_ref[...].astype(jnp.bfloat16)


def in_forward(x, w, table):
    (rows, depth), width = x.shape, w.shape[1]
    size = depth // 8
    return run(
        in_kernel, table, [x, w],
        [pl.BlockSpec((rows, size), lambda i, t: (0, i)), pl.BlockSpec((size, width), lambda i, t: (i, 0))],
        [jax.ShapeDtypeStruct((rows, width), dtype) for dtype in (jnp.float32, jnp.bfloat16)],
        [pl.BlockSpec((rows, width), lambda i, t: (0, 0))] * 2,
        depth // size, (2 * rows * depth * width, 4 * depth * width + 2 * rows * depth),
    )


def select_piece(step, steps_per_piece, piece_refs):
    value = piece_refs[0][...]
    for idx in range(1, len(piece_refs)):
        value = jnp.where(step >= idx * steps_per_piece, piece_refs[idx][...], value)
    return value


def updated(w_ref, m_ref, grad, step_size):
    new_m = MOMENTUM * m_ref[...] + grad.astype(jnp.float32).reshape(m_ref.shape)
    new_w = w_ref[...] - step_size * new_m
    return new_w, new_m


def rows_kernel(count, per, step_size, has_h, has_old, *refs):
    refs = list(refs)
    refs.pop(0)
    x_ref = refs.pop(0)
    w_ref, m_ref = refs.pop(0), refs.pop(0)
    pieces = [refs.pop(0) for _ in range(count)]
    h_ref = refs.pop(0) if has_h else None
    if has_old:
        refs.pop(0), refs.pop(0)
    new_w_ref, new_m_ref, out_ref = refs
    step = pl.program_id(0)

    @pl.when(step == 0)
    def _():
        out_ref[...] = h_ref[...] if has_h else jnp.zeros_like(out_ref)

    grad = select_piece(step, per, pieces)
    lead = (0,) * (len(w_ref.shape) - 2)
    for lo in range(0, out_ref.shape[1], 2 * CHUNK):
        at = slice(lo, lo + 2 * CHUNK)
        place = lead + (slice(None), at)
        new_m = MOMENTUM * m_ref[place] + grad[:, at].astype(jnp.float32)
        new_w = w_ref[place] - step_size * new_m
        new_w_ref[place] = new_w
        new_m_ref[place] = new_m
        out_ref[:, at] += jnp.dot(x_ref[...], new_w.astype(jnp.bfloat16), preferred_element_type=jnp.float32)


def update_rows(x, w, m, layer, pieces, bases, h, old, step_size):
    count, rows = len(pieces), x.shape[0]
    height, width = pieces[0].shape
    per = height // BLOCK
    stacked = w.ndim == 3
    table = jnp.stack(bases) * per

    def where(i, t):
        return t[i // per] + i % per

    lead = (1,) if stacked else ()
    at = (lambda i, t: (layer, where(i, t), 0)) if stacked else (lambda i, t: (where(i, t), 0))
    w_spec = pl.BlockSpec(lead + (BLOCK, width), at)
    in_specs = [pl.BlockSpec((rows, BLOCK), lambda i, t: (0, where(i, t))), w_spec, w_spec]
    in_specs += [
        pl.BlockSpec((BLOCK, width), lambda i, t, j=j: (jnp.clip(i - j * per, 0, per - 1), 0)) for j in range(count)
    ]
    h_spec = pl.BlockSpec((rows, width), lambda i, t: (0, 0))
    operands = [x, w, m, *pieces]
    aliases = {}
    if h is not None:
        operands.append(h)
        in_specs.append(h_spec)
    if old is not None:
        aliases = {len(operands) + 1: 0, len(operands) + 2: 1}
        operands += list(old)
        in_specs += [pl.BlockSpec(memory_space=pl.ANY)] * 2
    steps = count * per
    size = steps * BLOCK * width
    full = jax.ShapeDtypeStruct(w.shape, jnp.float32)
    new_w, new_m, out = run(
        functools.partial(rows_kernel, count, per, step_size, h is not None, old is not None), table, operands,
        in_specs, [full, full, jax.ShapeDtypeStruct((rows, width), jnp.float32)], [w_spec, w_spec, h_spec],
        steps, (2 * rows * size, 18 * size), aliases=aliases,
    )
    return (new_w, new_m), out


def cols_kernel(count, per, step_size, has_old, *refs):
    refs = list(refs)
    refs.pop(0)
    h_ref = refs.pop(0)
    w_ref, m_ref = refs.pop(0), refs.pop(0)
    pieces = [refs.pop(0) for _ in range(count)]
    new_w_ref, new_m_ref, act_ref, low_ref = refs[has_old:]
    step = pl.program_id(0)

    @pl.when(step == 0)
    def _():
        low_ref[...] = h_ref[...].astype(jnp.bfloat16)

    new_w, new_m = updated(w_ref, m_ref, select_piece(step, per, pieces), step_size)
    new_w_ref[...] = new_w
    new_m_ref[...] = new_m
    low = new_w.reshape(new_w.shape[-2:]).astype(jnp.bfloat16)
    pre = jnp.dot(low_ref[...], low, preferred_element_type=jnp.float32)
    act_ref[...] = gelu_tanh(pre).astype(jnp.bfloat16)


def update_cols(h, w, m, layer, pieces, bases, old, step_size):
    count, rows = len(pieces), h.shape[0]
    depth, width = pieces[0].shape
    per = width // BLOCK
    table = jnp.stack(bases) * per

    def where(i, t):
        return t[i // per] + i % per

    w_spec = pl.BlockSpec((1, depth, BLOCK), lambda i, t: (layer, 0, where(i, t)))
    a_spec = pl.BlockSpec((rows, BLOCK), lambda i, t: (0, where(i, t)))
    in_specs = [pl.BlockSpec((rows, depth), lambda i, t: (0, 0)), w_spec, w_spec]
    in_specs += [
        pl.BlockSpec((depth, BLOCK), lambda i, t, j=j: (0, jnp.clip(i - j * per, 0, per - 1))) for j in range(count)
    ]
    operands = [h, w, m, *pieces]
    aliases = {}
    kept = [(out_idx, value) for out_idx, value in enumerate(old) if value is not None]
    for out_idx, value in kept:
        aliases[len(operands) + 1] = out_idx
        operands.append(value)
        in_specs.append(pl.BlockSpec(memory_space=pl.ANY))
    steps = count * per
    size = steps * BLOCK * depth
    full = jax.ShapeDtypeStruct(w.shape, jnp.float32)
    new_w, new_m, act = run(
        functools.partial(cols_kernel, count, per, step_size, len(kept)), table, operands,
        in_specs, [full, full, jax.ShapeDtypeStruct((rows, w.shape[2]), jnp.bfloat16)], [w_spec, w_spec, a_spec],
        steps, (2 * rows * size, 18 * size), [pltpu.VMEM((rows, depth), jnp.bfloat16)], aliases,
    )
    return (new_w, new_m), act


def solution(mesh):
    group_size = mesh.shape["data"]

    def device_steps(w_in, w_up, w_down, mom_in, mom_up, mom_down, x_now, y_now, x_next, y_next):
        local_rows, model_width = y_now.shape
        layer_count = w_up.shape[0]
        inner = w_up.shape[2]
        step_size = 4.0 * model_width / (inner * (layer_count + 1))
        along_x, along_y = Plan(2, 4, group_size), Plan(4, 2, group_size)

        halves = along_x.eighths() + [8 + idx for idx in along_y.eighths()]
        x_parts = split_cols(x_now, jnp.stack(halves), 8)
        up_plans, down_plans = [along_x, along_y], [along_y, along_x]
        in_wide = [along_x.exchange_wide(x_parts[:4]), along_y.exchange_wide(x_parts[4:])]

        h_state, h_low = in_forward(x_now, w_in, jnp.stack(halves))
        saved = []
        for layer in range(layer_count):
            up_plan, down_plan = up_plans[layer % 2], down_plans[layer % 2]
            up_near = up_plan.exchange_narrow(h_low)
            pre_act, *act_parts = up_forward(h_low, w_up, layer, down_plan.eighths())
            down_wide = down_plan.exchange_wide(act_parts)
            h_state, h_low = add_product(h_state, act_parts, w_down, layer, down_plan.eighths(), False)
            saved.append((up_near, down_wide, pre_act))
        cot_state = (h_state - y_now.astype(jnp.float32)) / (local_rows * group_size * model_width)

        def share(lhs, rhs):
            lhs, rhs = jnp.concatenate(lhs), jnp.concatenate(rhs)
            value = lax.dot_general(lhs, rhs, ROW_CONTRACT, preferred_element_type=jnp.float32)
            return value.astype(jnp.bfloat16)

        factors = [None] * layer_count
        cot_low = cot_state.astype(jnp.bfloat16)
        for layer in reversed(range(layer_count)):
            up_plan, down_plan = up_plans[layer % 2], down_plans[layer % 2]
            up_near, down_wide, pre_act = saved[layer]
            cot_near = down_plan.exchange_narrow(cot_low)
            pre_parts = down_backward(cot_low, w_down, layer, pre_act, up_plan.eighths())
            pre_wide = up_plan.exchange_wide(pre_parts)
            cot_state, cot_low = add_product(cot_state, pre_parts, w_up, layer, up_plan.eighths(), True)
            factors[layer] = (down_wide, cot_near, up_near, pre_wide)
        cot_near = [along_x.exchange_narrow(cot_low), along_y.exchange_narrow(cot_low)]

        up_sums, down_sums, in_sums = [None] * layer_count, [None] * layer_count, [None] * 2
        for layer in reversed(range(layer_count)):
            down_wide, near, up_near, pre_wide = factors[layer]
            up_sums[layer] = up_plans[layer % 2].reduce_piece(share(up_near, pre_wide), 1)
            down_sums[layer] = down_plans[layer % 2].reduce_piece(share(down_wide, near), 0)
        for part, plan in enumerate((along_x, along_y)):
            in_sums[part] = plan.reduce_piece(share(in_wide[part], cot_near[part]), 0)

        h_state, new_in, new_up, new_down = None, None, None, None
        groups = [plan.gather(own) for plan, own in zip((along_x, along_y), in_sums)]
        for idx in range(4):
            tagged = groups[0][idx] + [(value, base + 8) for value, base in groups[1][idx]]
            pieces, bases = zip(*tagged)
            new_in, h_state = update_rows(x_next, w_in, mom_in, 0, pieces, bases, h_state, new_in, step_size)
        for layer in range(layer_count):
            act_low, h_up = None, h_state
            up_groups = up_plans[layer % 2].gather(up_sums[layer])
            down_groups = down_plans[layer % 2].gather(down_sums[layer])

            def up_step(idx, new_up, act_low):
                pieces, bases = zip(*up_groups[idx])
                old = (None, None, act_low) if new_up is None else (*new_up, act_low)
                return update_cols(h_up, w_up, mom_up, layer, pieces, bases, old, step_size)

            def down_step(idx, new_down, h_state, act_low):
                pieces, bases = zip(*down_groups[idx])
                return update_rows(act_low, w_down, mom_down, layer, pieces, bases, h_state, new_down, step_size)

            for is_up, idx in UPDATE_ORDER:
                if is_up:
                    new_up, act_low = up_step(idx, new_up, act_low)
                else:
                    new_down, h_state = down_step(idx, new_down, h_state, act_low)
        loss_next = jnp.sum(jnp.square(h_state - y_next.astype(jnp.float32)), axis=1) / (2 * model_width)
        return (new_in[0], new_up[0], new_down[0], new_in[1], new_up[1], new_down[1], loss_next, h_state)

    param_spec = P()
    row_spec = P("data", None)

    return jax.shard_map(
        device_steps,
        mesh=mesh,
        in_specs=(param_spec,) * 6 + (row_spec,) * 4,
        out_specs=(param_spec,) * 6 + (P("data"), row_spec),
        check_vma=False,
    )
```
